32 devices in a mesh: pair: 4 (over x, core), aux: 8 (over z, y).
Axes of the slice: x: 2, y: 2, z: 4, core: 2. Of those that a mesh axis runs over, the one named last changes fastest.
Arguments:
- left_active: bfloat16 [40, 128, 61440], P('pair', None, 'aux'), may hold values from -0.375 to 0.375
- right_active: bfloat16 [40, 128, 61440], P('pair', None, 'aux'), may hold values from -0.375 to 0.375
- amps_active: bfloat16 [40, 128, 128], P('pair', 'aux'), may hold values from -0.5 to 0.5
- rank_active: int32 [40], P('pair'), may hold values from 80 to 128, as said below
- gap_active: float32 [40], P('pair'), may hold values from 0.5 to 2
- energy_active: float32 [40, 128], P('pair'), may hold values from 0.5 to 4
- intersect_active: bfloat16 [40, 4, 128, 128], P('pair'), may hold values from -0.75 to 0.75
- fock_active: float32 [40, 4], P('pair'), may hold values from -2 to 2
- neighbor_active: int32 [40, 4], P('pair'), may hold values from 0 to 39
- left_env: bfloat16 [16, 48, 61440], P('pair', None, 'aux'), may hold values from -0.375 to 0.375
- right_env: bfloat16 [16, 48, 61440], P('pair', None, 'aux'), may hold values from -0.375 to 0.375
- amps_env: bfloat16 [16, 48, 48], P('pair', 'aux'), may hold values from -0.875 to 0.875
- rank_env: int32 [16], P('pair'), may hold values from 24 to 48, as said below
- gap_env: float32 [16], P('pair'), may hold values from 0.5 to 2
- energy_env: float32 [16, 48], P('pair'), may hold values from 0.5 to 4
- intersect_env: bfloat16 [16, 4, 48, 48], P('pair'), may hold values from -1.25 to 1.25
- fock_env: float32 [16, 4], P('pair'), may hold values from -2 to 2
- neighbor_env: int32 [16, 4], P('pair'), may hold values from 0 to 15
Outputs:
- new_active: float32 [40, 128, 128], P('pair', 'aux')
- new_env: float32 [16, 48, 48], P('pair', 'aux')
The draws below stay inside these ranges and needn't reach their ends.
Inputs may be any that keep to these rules, and one draw needn't show every extreme that they name: `rank_active`: multiples of 8; the first active pair has rank 128. `rank_env`: multiples of 8; the first environment pair has rank 48.
All inputs are finite; a program needn't handle non-finite values.
Results may differ from the reference program's by a relative error of at most 0.0041.
Values may be sent and summed in bfloat16 or wider, within the bound.
A program may use at most 128 MiB of HBM per device.

```python
import math
import jax
import jax.numpy as jnp
from jax import lax

RA = 128
RE = 48
NAUX = 61440
NB = 4
PA = 40
PE = 16


def draw_rank_active(key, part):
    values = 8 * jax.random.randint(key, (PA,), RA * 5 // 64, RA // 8 + 1)
    return values.at[0].set(RA).astype(jnp.int32)


def draw_rank_env(key, part):
    values = 8 * jax.random.randint(key, (PE,), RE // 16, RE // 8 + 1)
    return values.at[0].set(RE).astype(jnp.int32)


def set_ends(array, key, least, high):
    longest = array.shape.index(max(array.shape))
    spots = []
    for shift in (0, 1):
        where = [jax.random.randint(jax.random.fold_in(key, axis), (), 0, length) for axis, length in enumerate(array.shape)]
        where[longest] = (where[longest] + shift) % array.shape[longest]
        spots.append(tuple(where))
    return array.at[spots[0]].set(least).at[spots[1]].set(high)


def block_scale(own_key, extent, shards, least, largest):
    factor_of = 1.0
    for position, blocks in shards:
        steps = jax.random.uniform(jax.random.fold_in(jax.random.fold_in(own_key, 6), position), (blocks,), jnp.float32, least / len(shards), largest / len(shards))
        factor_of = factor_of * jnp.repeat(jnp.exp(steps), extent[position] // blocks).reshape((-1,) + (1,) * (len(extent) - 1 - position))
    return factor_of


def normal_values(own_key, dims, width, most, pieces=(), held_as=jnp.bfloat16):
    factor_of = block_scale(own_key, dims, pieces, -0.22, 0.18) if pieces else 1.0
    entries = jax.random.normal(own_key, dims, jnp.float32) * width * factor_of
    return jnp.minimum(jnp.maximum(entries, -most), most).astype(held_as)


def setup_inputs(seed: int = 0) -> dict:
    key_list = jax.random.split(jax.random.key(seed), 19)
    left_active = normal_values(key_list[0], (PA, RA, NAUX), (NAUX ** -0.25), 0.375, ((0, 4), (2, 8)))
    right_active = normal_values(key_list[1], (PA, RA, NAUX), (NAUX ** -0.25), 0.375, ((0, 4), (2, 8)))
    amps_active = normal_values(key_list[2], (PA, RA, RA), (RA ** -0.5), 0.5, ((0, 4), (1, 8)))
    rank_active = draw_rank_active(jax.random.fold_in(key_list[18], 71), 0)
    gap_active = jnp.clip(jnp.exp(math.log(2.0) - 1.3862944 * jax.random.uniform(key_list[4], (PA,), jnp.float32) ** block_scale(key_list[4], (PA,), ((0, 4),), -0.2, 0.2)), 0.5, 2.0)
    energy_active = jnp.clip(jnp.exp(math.log(4.0) - 2.0794415 * jax.random.uniform(key_list[5], (PA, RA), jnp.float32) ** block_scale(key_list[5], (PA, RA), ((0, 4),), -0.2, 0.2)), 0.5, 4.0)
    intersect_active = normal_values(key_list[6], (PA, NB, RA, RA), (RA // 2) ** -0.5, 0.75, ((0, 4),))
    fock_active = jnp.clip(jax.random.uniform(key_list[7], (PA, NB), jnp.float32, -2.0, 2.0) * block_scale(key_list[7], (PA, NB), ((0, 4),), -0.4, 0.0), -2.0, 2.0)
    neighbor_active = set_ends(jax.random.randint(key_list[8], (PA, NB), 0, PA), jax.random.fold_in(key_list[8], 1), 0, PA - 1).astype(jnp.int32)
    left_env = normal_values(key_list[9], (PE, RE, NAUX), (NAUX ** -0.25), 0.375, ((0, 4), (2, 8)))
    right_env = normal_values(key_list[10], (PE, RE, NAUX), (NAUX ** -0.25), 0.375, ((0, 4), (2, 8)))
    amps_env = normal_values(key_list[11], (PE, RE, RE), (RE ** -0.5), 0.875, ((0, 4), (1, 8)))
    rank_env = draw_rank_env(jax.random.fold_in(key_list[18], 71), 0)
    gap_env = jnp.clip(jnp.exp(math.log(2.0) - 1.3862944 * jax.random.uniform(key_list[13], (PE,), jnp.float32) ** block_scale(key_list[13], (PE,), ((0, 4),), -0.2, 0.2)), 0.5, 2.0)
    energy_env = jnp.clip(jnp.exp(math.log(4.0) - 2.0794415 * jax.random.uniform(key_list[14], (PE, RE), jnp.float32) ** block_scale(key_list[14], (PE, RE), ((0, 4),), -0.2, 0.2)), 0.5, 4.0)
    intersect_env = normal_values(key_list[15], (PE, NB, RE, RE), (RE // 2) ** -0.5, 1.25, ((0, 4),))
    fock_env = jnp.clip(jax.random.uniform(key_list[16], (PE, NB), jnp.float32, -2.0, 2.0) * block_scale(key_list[16], (PE, NB), ((0, 4),), -0.4, 0.0), -2.0, 2.0)
    neighbor_env = set_ends(jax.random.randint(key_list[17], (PE, NB), 0, PE), jax.random.fold_in(key_list[17], 1), 0, PE - 1).astype(jnp.int32)
    return dict(left_active=left_active, right_active=right_active, amps_active=amps_active, rank_active=rank_active, gap_active=gap_active, energy_active=energy_active, intersect_active=intersect_active, fock_active=fock_active, neighbor_active=neighbor_active, left_env=left_env, right_env=right_env, amps_env=amps_env, rank_env=rank_env, gap_env=gap_env, energy_env=energy_env, intersect_env=intersect_env, fock_env=fock_env, neighbor_env=neighbor_env)


HIGHEST = lax.Precision.HIGHEST


def rank_masks(pair_ranks, full_width):
    positions = jnp.arange(full_width, dtype=jnp.int32)
    return (positions[None, :, None] < pair_ranks[:, None, None]) & (positions[None, None, :] < pair_ranks[:, None, None])


def update_level(left_ints, right_ints, amplitudes, pair_ranks, pair_gaps, energy, intersect, fock_weights, neighbor, with_ladder):
    full_width = amplitudes.shape[1]
    inside = rank_masks(pair_ranks, full_width)
    masked = jnp.where(inside, amplitudes, jnp.zeros_like(amplitudes))

    def one_pair(pair_items):
        left_pair, right_pair, amp_pair, over_pair, fock_pair, neigh_pair = pair_items
        summed_terms = jnp.dot(left_pair, right_pair.T, preferred_element_type=jnp.float32)
        if with_ladder:
            cross_left = jnp.dot(amp_pair.T, left_pair, preferred_element_type=jnp.float32).astype(jnp.bfloat16)
            cross_right = jnp.dot(amp_pair, right_pair, preferred_element_type=jnp.float32).astype(jnp.bfloat16)
            summed_terms = summed_terms + jnp.dot(cross_left, right_pair.T, preferred_element_type=jnp.float32)
            summed_terms = summed_terms + jnp.dot(cross_left, cross_right.T, preferred_element_type=jnp.float32)
        near_amps = masked[neigh_pair]
        half_product = jnp.einsum('krs,kst->krt', over_pair, near_amps, preferred_element_type=jnp.float32)
        full_product = jnp.einsum('krt,kut->kru', half_product, over_pair.astype(jnp.float32), precision=HIGHEST)
        return summed_terms + jnp.einsum('k,kru->ru', fock_pair, full_product, precision=HIGHEST)

    residual = lax.map(one_pair, (left_ints, right_ints, masked, intersect, fock_weights, neighbor))
    denominator = energy[:, :, None] + energy[:, None, :] + pair_gaps[:, None, None]
    return jnp.where(inside, masked.astype(jnp.float32) - residual / denominator, jnp.float32(0.0))


def reference(left_active, right_active, amps_active, rank_active, gap_active, energy_active, intersect_active, fock_active, neighbor_active, left_env, right_env, amps_env, rank_env, gap_env, energy_env, intersect_env, fock_env, neighbor_env):
    new_active = update_level(left_active, right_active, amps_active, rank_active, gap_active, energy_active, intersect_active, fock_active, neighbor_active, True)
    new_env = update_level(left_env, right_env, amps_env, rank_env, gap_env, energy_env, intersect_env, fock_env, neighbor_env, False)
    return (new_active, new_env)
```

```python
import functools

import jax
import jax.numpy as jnp
from jax import lax
from jax.experimental import pallas as pl
from jax.experimental.pallas import tpu as pltpu
from jax.sharding import PartitionSpec as P

BF = jnp.bfloat16
F32 = jnp.float32
LANES = 128
AHEAD = 4


def dot_nt(x, y):
    return lax.dot_general(x, y, (((1,), (1,)), ((), ())), preferred_element_type=F32)


def split(x):
    hi = x.astype(BF)
    return hi, (x - hi.astype(F32)).astype(BF)


def iota2(shape, dim):
    return lax.broadcasted_iota(jnp.int32, shape, dim)


def couple(over, near, fock, place, rows, step):
    count = len(over)
    width = over[0].shape[1]
    pick = (iota2((step, width), 1) == place * rows + iota2((step, width), 0)) & (
        iota2((step, width), 0) < rows
    )
    pick = jnp.where(pick, F32(1.0), F32(0.0))
    both = None
    for k in range(count):
        above = [jnp.zeros((step * k, width), F32)] if k else []
        below = [jnp.zeros((LANES - step * (k + 1), width), F32)]
        weights = jnp.concatenate(above + [near[k]] + below + above + [pick] + below, axis=0)
        part = dot_nt(over[k], weights.astype(BF))
        both = part if both is None else both + part
    lane = iota2((1, LANES), 1)
    scale = jnp.zeros((1, LANES), F32)
    for k in range(count):
        scale = jnp.where((lane >= step * k) & (lane < step * (k + 1)), fock[k], scale)
    hi, lo = split(both[:, :LANES] * scale)
    cols = both[:, LANES:].astype(BF)
    return dot_nt(jnp.concatenate([cols, cols], axis=1), jnp.concatenate([hi, lo], axis=1))


def kernel(
    n_pair, n_aux,
    la, ra, aa, rka, gpa, ena, ina, fka, nba,
    le, re, ae, rke, gpe, ene, ine, fke, nbe,
    oa, oe,
    lbuf, rbuf, lebuf, rebuf, inbuf,
    mine, own, around, mine_e, around_e,
    terms, out_a, in_a, terms_e, out_e, in_e, den, den_e,
    lr_sem, lre_sem, in_sem,
    own_send, own_recv, pair_send, pair_recv, paire_send, paire_recv,
    a_send, a_recv, e_send, e_recv,
):
    pairs, rows, full = aa.shape
    pairs_e, rows_e, full_e = ae.shape
    pad_e = mine_e.shape[1]
    count = nba.shape[1]
    me = lax.axis_index("aux")
    my_pair = lax.axis_index("pair")

    def load_lr(p):
        return (
            pltpu.make_async_copy(la.at[p], lbuf.at[p], lr_sem.at[p, 0]),
            pltpu.make_async_copy(ra.at[p], rbuf.at[p], lr_sem.at[p, 1]),
        )

    load_e = (
        pltpu.make_async_copy(le, lebuf, lre_sem.at[0]),
        pltpu.make_async_copy(re, rebuf, lre_sem.at[1]),
    )
    load_in = pltpu.make_async_copy(ina, inbuf, in_sem)
    for copy in load_e:
        copy.start()
    load_in.start()
    for p in range(min(AHEAD, pairs)):
        for copy in load_lr(p):
            copy.start()

    barrier = pltpu.get_barrier_semaphore()
    for d in range(1, n_aux):
        pl.semaphore_signal(barrier, inc=1, device_id={"aux": lax.rem(me + d, n_aux)}, device_id_type=pl.DeviceIdType.MESH)
    for d in range(1, n_pair):
        pl.semaphore_signal(barrier, inc=1, device_id={"pair": lax.rem(my_pair + d, n_pair)}, device_id_type=pl.DeviceIdType.MESH)

    def inside(rank, start, shape):
        return (start + iota2(shape, 0) < rank) & (iota2(shape, 1) < rank)

    for p in range(pairs):
        keep = inside(rka[p], me * rows, (rows, full))
        block = jnp.where(keep, aa[p].astype(F32), F32(0.0)).astype(BF)
        mine[p] = block
        own[me, p] = block
        around[my_pair * pairs + p] = block
    mine_e[...] = jnp.zeros(mine_e.shape, F32)
    for p in range(pairs_e):
        keep = inside(rke[p], me * rows_e, (rows_e, full_e))
        mine_e[p, :rows_e, :full_e] = jnp.where(keep, ae[p].astype(F32), F32(0.0))
    for p in range(pairs_e):
        around_e[my_pair * pairs_e + p] = mine_e[p]
    out_e[...] = jnp.zeros(out_e.shape, F32)

    def to_own(d, slot):
        return pltpu.make_async_remote_copy(
            src_ref=mine, dst_ref=own.at[slot],
            send_sem=own_send.at[d - 1], recv_sem=own_recv.at[d - 1],
            device_id={"aux": lax.rem(me + d, n_aux)}, device_id_type=pl.DeviceIdType.MESH,
        )

    def to_pair(d, slot):
        return pltpu.make_async_remote_copy(
            src_ref=mine, dst_ref=around.at[pl.ds(slot * pairs, pairs)],
            send_sem=pair_send.at[d - 1], recv_sem=pair_recv.at[d - 1],
            device_id={"pair": lax.rem(my_pair + d, n_pair)}, device_id_type=pl.DeviceIdType.MESH,
        )

    def to_pair_e(d, slot):
        return pltpu.make_async_remote_copy(
            src_ref=mine_e, dst_ref=around_e.at[pl.ds(slot * pairs_e, pairs_e)],
            send_sem=paire_send.at[d - 1], recv_sem=paire_recv.at[d - 1],
            device_id={"pair": lax.rem(my_pair + d, n_pair)}, device_id_type=pl.DeviceIdType.MESH,
        )

    pl.semaphore_wait(barrier, n_aux - 1 + n_pair - 1)
    for d in range(1, n_pair):
        to_pair(d, my_pair).start()
        to_pair_e(d, my_pair).start()
    for d in range(1, n_aux):
        to_own(d, me).start()

    def denominators(energy, gap, start, height, wide):
        line = energy + jnp.zeros((height, wide), F32)
        diag = iota2((height, wide), 1) == start + iota2((height, wide), 0)
        mine_rows = jnp.sum(jnp.where(diag, line, F32(0.0)), axis=1, keepdims=True)
        return line + mine_rows + gap

    for p in range(pairs):
        den[p] = denominators(ena[pl.ds(p, 1), :], gpa[p], me * rows, rows, full)
    for p in range(pairs_e):
        den_e[p] = denominators(ene[pl.ds(p, 1), :], gpe[p], me * rows_e, rows_e, full_e)

    for copy in load_e:
        copy.wait()
    for p in range(pairs_e):
        terms_e[p] = dot_nt(lebuf[p], rebuf[p])

    def a_copy(d, p):
        peer = lax.rem(me + d, n_aux)
        return pltpu.make_async_remote_copy(
            src_ref=out_a.at[peer, p], dst_ref=in_a.at[d - 1, p],
            send_sem=a_send.at[d - 1], recv_sem=a_recv.at[d - 1],
            device_id={"aux": peer}, device_id_type=pl.DeviceIdType.MESH,
        )

    def e_copy(d):
        peer = lax.rem(me + d, n_aux)
        return pltpu.make_async_remote_copy(
            src_ref=out_e.at[peer], dst_ref=in_e.at[d - 1],
            send_sem=e_send.at[d - 1], recv_sem=e_recv.at[d - 1],
            device_id={"aux": peer}, device_id_type=pl.DeviceIdType.MESH,
        )

    def send_pair(p):
        for d in range(1, n_aux):
            a_copy(d, p).start()

    def step(p, carry):
        @pl.when(p + AHEAD < pairs)
        def _():
            for copy in load_lr(p + AHEAD):
                copy.start()

        for copy in load_lr(p):
            copy.wait()
        base = dot_nt(lbuf[p], rbuf[p])

        @pl.when(p == 0)
        def _():
            for d in range(1, n_pair):
                slot = lax.rem(my_pair + n_pair - d, n_pair)
                to_pair(d, slot).wait_recv()
                to_pair_e(d, slot).wait_recv()
            for d in range(1, n_aux):
                to_own(d, lax.rem(me + n_aux - d, n_aux)).wait_recv()
            load_in.wait()

        amps = own[:, p].astype(F32).reshape(full, full)
        flat = amps.astype(BF)
        turned = amps.T.astype(BF)
        hi, lo = split(base)
        half = base + (dot_nt(hi, flat) + dot_nt(lo, flat))
        hi, lo = split(half)
        total = base + jnp.dot(
            jnp.concatenate([turned, turned], axis=1),
            jnp.concatenate([hi, lo], axis=0),
            preferred_element_type=F32,
        )
        total = total + couple(
            [inbuf[p, k] for k in range(count)],
            [around[nba[p, k]].astype(F32) for k in range(count)],
            [fka[p, k] for k in range(count)],
            me, rows, rows,
        )
        terms[p] = total.reshape(n_aux, rows, full)
        for j in range(n_aux):
            out_a[j, p] = total[j * rows : (j + 1) * rows].astype(BF)

        @pl.when(p > 0)
        def _():
            send_pair(p - 1)

        @pl.when(p == 1)
        def _():
            for q in range(pairs_e):
                terms_e[q] = terms_e[q] + couple(
                    [ine[q, k] for k in range(count)],
                    [around_e[nbe[q, k]][:, :full_e] for k in range(count)],
                    [fke[q, k] for k in range(count)],
                    me, rows_e, pad_e,
                )
                for j in range(n_aux):
                    out_e[j, q, :rows_e, :full_e] = terms_e[q, j * rows_e : (j + 1) * rows_e, :]

        @pl.when(p == 2)
        def _():
            for d in range(1, n_aux):
                e_copy(d).start()

        return carry

    lax.fori_loop(0, pairs, step, 0)
    send_pair(pairs - 1)

    for d in range(1, n_aux):
        e_copy(d).wait_recv()
    for p in range(pairs_e):
        total = out_e[me, p]
        for d in range(1, n_aux):
            total = total + in_e[d - 1, p]
        keep = inside(rke[p], me * rows_e, (rows_e, full_e))
        oe[p] = jnp.where(
            keep, mine_e[p, :rows_e, :full_e] - total[:rows_e, :full_e] / den_e[p], F32(0.0)
        )

    for d in range(1, n_aux):
        pltpu.make_async_copy(in_a.at[d - 1], in_a.at[d - 1], a_recv.at[d - 1]).wait()
    for p in range(pairs):
        total = terms[p, me]
        for d in range(1, n_aux):
            total = total + in_a[d - 1, p].astype(F32)
        keep = inside(rka[p], me * rows, (rows, full))
        oa[p] = jnp.where(keep, mine[p].astype(F32) - total / den[p], F32(0.0))

    for d in range(1, n_pair):
        to_pair(d, my_pair).wait_send()
        to_pair_e(d, my_pair).wait_send()
    for d in range(1, n_aux):
        to_own(d, me).wait_send()
        e_copy(d).wait_send()
        pltpu.make_async_copy(in_a.at[d - 1], in_a.at[d - 1], a_send.at[d - 1]).wait()


def shards(n_pair, n_aux, *args):
    la, ra, aa = args[:3]
    ina = args[6]
    le, re, ae = args[9:12]
    pairs, rows, full = aa.shape
    pairs_e, rows_e, full_e = ae.shape
    pad_e = -(-rows_e // 8) * 8
    vmem = pl.BlockSpec(memory_space=pltpu.VMEM)
    smem = pl.BlockSpec(memory_space=pltpu.SMEM)
    hbm = pl.BlockSpec(memory_space=pl.ANY)
    dma = pltpu.SemaphoreType.DMA
    level = [hbm, hbm, vmem, smem, smem, vmem]
    return pl.pallas_call(
        functools.partial(kernel, n_pair, n_aux),
        out_shape=(
            jax.ShapeDtypeStruct(aa.shape, F32),
            jax.ShapeDtypeStruct(ae.shape, F32),
        ),
        in_specs=level + [hbm, smem, smem] + level + [vmem, smem, smem],
        out_specs=(vmem, vmem),
        scratch_shapes=[
            pltpu.VMEM(la.shape, BF),
            pltpu.VMEM(ra.shape, BF),
            pltpu.VMEM(le.shape, BF),
            pltpu.VMEM(re.shape, BF),
            pltpu.VMEM(ina.shape, BF),
            pltpu.VMEM((pairs, rows, full), BF),
            pltpu.VMEM((n_aux, pairs, rows, full), BF),
            pltpu.VMEM((n_pair * pairs, rows, full), BF),
            pltpu.VMEM((pairs_e, pad_e, LANES), F32),
            pltpu.VMEM((n_pair * pairs_e, pad_e, LANES), F32),
            pltpu.VMEM((pairs, n_aux, rows, full), F32),
            pltpu.VMEM((n_aux, pairs, rows, full), BF),
            pltpu.VMEM((n_aux - 1, pairs, rows, full), BF),
            pltpu.VMEM((pairs_e, full_e, full_e), F32),
            pltpu.VMEM((n_aux, pairs_e, pad_e, LANES), F32),
            pltpu.VMEM((n_aux - 1, pairs_e, pad_e, LANES), F32),
            pltpu.VMEM((pairs, rows, full), F32),
            pltpu.VMEM((pairs_e, rows_e, full_e), F32),
            dma((pairs, 2)),
            dma((2,)),
            dma,
            dma((n_aux - 1,)),
            dma((n_aux - 1,)),
            dma((n_pair - 1,)),
            dma((n_pair - 1,)),
            dma((n_pair - 1,)),
            dma((n_pair - 1,)),
            dma((n_aux - 1,)),
            dma((n_aux - 1,)),
            dma((n_aux - 1,)),
            dma((n_aux - 1,)),
        ],
        compiler_params=pltpu.CompilerParams(
            collective_id=0, has_side_effects=True, vmem_limit_bytes=60 * 1024 * 1024
        ),
        name="update",
    )(*args)


def solution(mesh):
    n_pair, n_aux = mesh.shape["pair"], mesh.shape["aux"]
    level = (
        P("pair", None, "aux"),
        P("pair", None, "aux"),
        P("pair", "aux", None),
        P("pair"),
        P("pair"),
        P("pair", None),
        P("pair", None, None, None),
        P("pair", None),
        P("pair", None),
    )
    return jax.shard_map(
        functools.partial(shards, n_pair, n_aux),
        mesh=mesh,
        in_specs=level + level,
        out_specs=(P("pair", "aux", None), P("pair", "aux", None)),
        check_vma=False,
    )
```
